32 devices in a mesh: tok: 16 (over z, y, core), tp: 2 (over x).
Axes of the slice: x: 2, y: 2, z: 4, core: 2. Of those that a mesh axis runs over, the one named last changes fastest.
Arguments:
- hidden: bfloat16 [1536, 8192], P('tok'), may hold values from -2600 to 2600
- norm_gain: float32 [8192], replicated, may hold values from 0.5 to 1.5
- w_query: bfloat16 [8192, 4096], P('tok', 'tp'), may hold values from -1 to 1
- w_key: bfloat16 [8192, 1024], P('tok', 'tp'), may hold values from -1 to 1
- w_value: bfloat16 [8192, 1024], P('tok', 'tp'), may hold values from -0.0625 to 0.0625
- doc_ids: int32 [1536], P('tok'), may hold values from 0 to 3, as said below
Outputs:
- attended: bfloat16 [1536, 4096], P('tok', 'tp')
- out_scale: float32 [4096], P('tp')
- folded_gain: float32 [8192], P(('tok', 'tp'))
- codes_query: float32 [8192, 4096], P(('tok', 'tp'))
- codes_key: float32 [8192, 1024], P(('tok', 'tp'))
- codes_value: float32 [8192, 1024], P(('tok', 'tp'))
- scale_query: float32 [4096], P('tp')
- scale_key: float32 [1024], P('tp')
- scale_value: float32 [1024], P('tp')
The draws below stay inside these ranges and needn't reach their ends.
Inputs may be any that keep to these rules, and one draw needn't show every extreme that they name: doc_ids never falls along the tokens; each of the 4 documents holds 1 to 1152 tokens and one holds exactly 1152.
All inputs are finite; a program needn't handle non-finite values. Where the reference program divides by a largest or mean magnitude, that divisor is 1e-20 or more.
Results may differ from the reference program's by a relative error of at most 0.005.
The reference program's roundings to bfloat16 on the way (of `normed` and `value`) count: a program that leaves them out, or rounds other values in their place, can miss the bound.
Values may be sent and summed in bfloat16 or wider, within the bound.
A program may use at most 128 MiB of HBM per device.

```python
import math
import jax
import jax.numpy as jnp
from jax import lax

D = 8192
HEAD = 128
KVH = 8
QHEADS = 32
DOCS = 4
TOKENS = 1536
DOC_MOST = 1152


pair_count = 6


strengths = (0.75, 0.55, 0.35, 0.75, 0.55, 0.35)


planted_entry = 1.0


def document_layout(key):
    folded = jax.random.fold_in(key, 5151)
    key_where, key_cuts = jax.random.split(folded, 2)
    short_total = TOKENS - DOC_MOST
    long_place = jax.random.randint(key_where, (), 0, DOCS)
    cut_order = jax.random.permutation(key_cuts, short_total - 1)[:DOCS - 2] + 1
    cuts = jnp.sort(cut_order)
    bounds = jnp.concatenate([jnp.zeros((1,), jnp.int32), cuts.astype(jnp.int32), jnp.full((1,), short_total, jnp.int32)])
    shorts = bounds[1:] - bounds[:-1]
    order = jnp.arange(DOCS, dtype=jnp.int32)
    short_index = jnp.clip(order - (order > long_place).astype(jnp.int32), 0, DOCS - 2)
    lengths = jnp.where(order == long_place, DOC_MOST, shorts[short_index]).astype(jnp.int32)
    ends = jnp.cumsum(lengths).astype(jnp.int32)
    long_start = ends[long_place] - DOC_MOST
    return (ends, long_start)


def planted_layout(key):
    folded = jax.random.fold_in(key, 4242)
    key_perm, key_place, key_sign = jax.random.split(folded, 3)
    channels = jax.random.permutation(key_perm, D)[:3 * pair_count]
    ends, long_start = document_layout(key)
    stride = TOKENS // 4 // pair_count
    offsets = jax.random.randint(key_place, (pair_count,), 1, stride)
    later = long_start + TOKENS // 2 + jnp.arange(pair_count, dtype=jnp.int32) * stride + offsets
    reach = jnp.where(jnp.arange(pair_count) % 2 == 0, TOKENS // 2, 1)
    earlier = later - reach
    signs = jnp.where(jax.random.bernoulli(key_sign, 0.5, (KVH, HEAD)), 1.0, -1.0)
    half_head = HEAD // 2
    band_size = max(HEAD // 32, 2)
    band_start = half_head - band_size
    within = jnp.arange(HEAD) % half_head
    band = ((within >= band_start) & (within < band_start + band_size)).astype(jnp.float32)
    return (channels, later, earlier, signs * band[None, :])


def draw_doc_ids(key, part):
    ends, long_start = document_layout(key)
    token_index = jnp.arange(TOKENS, dtype=jnp.int32)
    return jnp.sum((token_index[:, None] >= ends[None, :DOCS - 1]).astype(jnp.int32), axis=1).astype(jnp.int32)


def main_rows(channels):
    row_index = jnp.arange(D)[:, None]
    is_main = jnp.any(row_index == channels[None, :pair_count], axis=1)
    is_extra = jnp.any(row_index == channels[None, pair_count:], axis=1)
    return (is_main, is_extra)


def drawn_weight(key, salt, columns):
    values = jnp.clip(jax.random.normal(jax.random.fold_in(key, salt), (D, columns), jnp.float32), -4.0, 4.0) / math.sqrt(D)
    return jnp.clip(values, -planted_entry, planted_entry)


def draw_w_query(key, part):
    values = drawn_weight(key, 11, QHEADS * HEAD)
    channels, later, earlier, pattern = planted_layout(key)
    is_main, is_extra = main_rows(channels)
    pattern_row = jnp.repeat(pattern, QHEADS // KVH, axis=0).reshape(QHEADS * HEAD)
    values = jnp.where(is_main[:, None], pattern_row[None, :], jnp.where(is_extra[:, None], 0.0, values))
    return values.astype(jnp.bfloat16)


def draw_w_key(key, part):
    values = drawn_weight(key, 12, KVH * HEAD)
    channels, later, earlier, pattern = planted_layout(key)
    is_main, is_extra = main_rows(channels)
    pattern_row = pattern.reshape(KVH * HEAD)
    values = jnp.where(is_main[:, None], pattern_row[None, :], jnp.where(is_extra[:, None], 0.0, values))
    return values.astype(jnp.bfloat16)


def draw_norm_gain(key, part):
    key_gain = jax.random.fold_in(key, 31)
    channels, later, earlier, pattern = planted_layout(key)
    is_main, is_extra = main_rows(channels)
    nearby = jax.random.uniform(jax.random.fold_in(key, 32), (D,), jnp.float32, 0.95, 1.05)
    spread = 1.0 + 0.1 * jnp.clip(jax.random.normal(key_gain, (D,), jnp.float32), -5.0, 5.0)
    return jnp.where(is_main, nearby, spread)


def draw_hidden(key, part):
    key_base, key_channel = jax.random.split(key, 2)
    base = jnp.clip(jax.random.normal(key_base, (TOKENS, D), jnp.float32), -4.0, 4.0)
    channels, later, earlier, pattern = planted_layout(key)
    column_index = jnp.arange(D)[None, :]
    main_hot = (column_index == channels[:pair_count, None]).astype(jnp.float32)
    is_main_column = jnp.sum(main_hot, axis=0, keepdims=True) > 0.5
    channel = jnp.exp(jax.random.uniform(key_channel, (1, D), jnp.float32, 0.0, math.log(30.0)))
    channel = jnp.where(is_main_column, 1.0, channel)
    values = base * channel
    token_index = jnp.arange(TOKENS)[:, None]
    is_later = (token_index == later[None, :]).astype(jnp.float32)
    is_earlier = (token_index == earlier[None, :]).astype(jnp.float32)
    late_hot = (column_index == channels[pair_count:2 * pair_count, None]).astype(jnp.float32)
    early_hot = (column_index == channels[2 * pair_count:, None]).astype(jnp.float32)
    levels = jnp.array(strengths, jnp.float32)
    main_amp = jnp.sqrt(levels)[:, None]
    rest_amp = jnp.sqrt(1.0 - levels - 0.0025)[:, None]
    late_rows = main_amp * main_hot + rest_amp * late_hot
    early_rows = main_amp * main_hot + rest_amp * early_hot
    planted = math.sqrt(D) * (jnp.dot(is_later, late_rows, precision=lax.Precision.HIGHEST) + jnp.dot(is_earlier, early_rows, precision=lax.Precision.HIGHEST))
    chosen = jnp.sum(is_later + is_earlier, axis=1) > 0.5
    values = jnp.where(chosen[:, None], 0.05 * base + planted, values)
    return jnp.clip(values, -2600.0, 2600.0).astype(jnp.bfloat16)


def block_levels(key, shape, shards, smallest, top_value):
    def one(position, shards_of):
        heights = jax.random.uniform(jax.random.fold_in(jax.random.fold_in(key, 6), position), (shards_of,), jnp.float32, smallest / len(shards), top_value / len(shards))
        return jnp.repeat(jnp.exp(heights), shape[position] // shards_of).reshape((-1,) + (1,) * (len(shape) - position - 1))

    factor_of = one(*shards[0])
    for cut in shards[1:]:
        factor_of = factor_of * one(*cut)
    return factor_of


def normal_values(stream_key, shape, width, limit, shards=(), kind=jnp.bfloat16):
    values = jax.random.normal(stream_key, shape, jnp.float32) * width
    if len(shards) > 0:
        values = block_levels(stream_key, shape, shards, -0.22, 0.18) * values
    return jnp.clip(values, min=-limit, max=limit).astype(kind)


def setup_inputs(seed: int = 0) -> dict:
    key_list = jax.random.split(jax.random.key(seed), 7)
    hidden = draw_hidden(jax.random.fold_in(key_list[6], 71), 0)
    norm_gain = draw_norm_gain(jax.random.fold_in(key_list[6], 71), 0)
    w_query = draw_w_query(jax.random.fold_in(key_list[6], 71), 0)
    w_key = draw_w_key(jax.random.fold_in(key_list[6], 71), 0)
    w_value = normal_values(key_list[4], (D, KVH * HEAD), D ** -0.5, 0.0625, ((0, 16), (1, 2)))
    doc_ids = draw_doc_ids(jax.random.fold_in(key_list[6], 71), 0)
    return dict(hidden=hidden, norm_gain=norm_gain, w_query=w_query, w_key=w_key, w_value=w_value, doc_ids=doc_ids)


def rotate(states, positions):
    half = states.shape[-1] // 2
    inverse = jnp.exp(jnp.arange(half, dtype=jnp.float32) * (-2.0 * math.log(10000.0) / states.shape[-1]))
    angles = positions[:, None] * inverse[None, :]
    cosine = jnp.cos(angles)[:, None, :]
    sine = jnp.sin(angles)[:, None, :]
    first = states[..., :half]
    second = states[..., half:]
    return jnp.concatenate([first * cosine - second * sine, second * cosine + first * sine], axis=-1)

def quantize(smoothing, matrix):
    smoothed = smoothing[:, None] * matrix.astype(jnp.float32)
    column_scale = jnp.maximum(lax.optimization_barrier(jnp.max(jnp.abs(smoothed), axis=0)), 1e-05) / 127.0
    return (smoothed / column_scale[None, :], column_scale)

def reference(hidden, norm_gain, w_query, w_key, w_value, doc_ids):
    tokens = hidden.shape[0]
    states = hidden.astype(jnp.float32)
    normed = (states * lax.rsqrt(lax.optimization_barrier(jnp.mean(states * states, axis=1, keepdims=True)) + 1e-05) * norm_gain[None, :]).astype(jnp.bfloat16)
    input_peak = lax.optimization_barrier(jnp.max(jnp.abs(normed.astype(jnp.float32)), axis=0))
    positions = jnp.arange(tokens, dtype=jnp.float32)
    query = rotate(jnp.dot(normed, w_query, preferred_element_type=jnp.float32).reshape(tokens, QHEADS, HEAD), positions).astype(jnp.bfloat16)
    key = rotate(jnp.dot(normed, w_key, preferred_element_type=jnp.float32).reshape(tokens, KVH, HEAD), positions).astype(jnp.bfloat16)
    value = jnp.dot(normed, w_value, preferred_element_type=jnp.float32).astype(jnp.bfloat16).reshape(tokens, KVH, HEAD)
    group_size = QHEADS // KVH
    index = jnp.arange(tokens, dtype=jnp.int32)
    allowed = (doc_ids[:, None] == doc_ids[None, :]) & (index[None, :] <= index[:, None])
    score_scale = 1.0 / math.sqrt(HEAD)

    def one_head(head_index):
        query_head = lax.dynamic_index_in_dim(query, head_index, 1, keepdims=False)
        key_head = lax.dynamic_index_in_dim(key, head_index // group_size, 1, keepdims=False)
        value_head = lax.dynamic_index_in_dim(value, head_index // group_size, 1, keepdims=False)
        scores = jnp.dot(query_head, key_head.T, preferred_element_type=jnp.float32) * score_scale
        scores = jnp.where(allowed, scores, -1e+30)
        highest = lax.optimization_barrier(jnp.max(scores, axis=1, keepdims=True))
        weights = jnp.where(allowed, jnp.exp(scores - highest), 0.0)
        totals = lax.optimization_barrier(jnp.sum(weights, axis=1, keepdims=True))
        return jnp.dot(weights.astype(jnp.bfloat16), value_head, preferred_element_type=jnp.float32) / totals
    heads = lax.map(one_head, jnp.arange(QHEADS, dtype=jnp.int32))
    attended = heads.transpose(1, 0, 2).reshape(tokens, QHEADS * HEAD).astype(jnp.bfloat16)
    out_scale = lax.optimization_barrier(jnp.max(jnp.abs(attended.astype(jnp.float32)), axis=0))
    weight_peak = jnp.maximum(jnp.maximum(lax.optimization_barrier(jnp.max(jnp.abs(w_query.astype(jnp.float32)), axis=1)), lax.optimization_barrier(jnp.max(jnp.abs(w_key.astype(jnp.float32)), axis=1))), lax.optimization_barrier(jnp.max(jnp.abs(w_value.astype(jnp.float32)), axis=1)))
    smoothing = jnp.sqrt(jnp.maximum(input_peak, 1e-05)) / jnp.sqrt(jnp.maximum(weight_peak, 1e-05))
    folded_gain = norm_gain / smoothing
    codes_query, scale_query = quantize(smoothing, w_query)
    codes_key, scale_key = quantize(smoothing, w_key)
    codes_value, scale_value = quantize(smoothing, w_value)
    return (attended, out_scale, folded_gain, codes_query, codes_key, codes_value, scale_query, scale_key, scale_value)
```

```python
import math

import jax
import jax.numpy as jnp
from jax import lax
from jax.sharding import PartitionSpec as P

HEAD = 128
KVH = 8
QHEADS = 32


def rotate(states, positions):
    half = states.shape[-1] // 2
    inverse = jnp.exp(
        jnp.arange(half, dtype=jnp.float32) * (-2.0 * math.log(10000.0) / states.shape[-1])
    )
    angles = positions[:, None] * inverse[None, :]
    cosine = jnp.cos(angles)[:, None, :]
    sine = jnp.sin(angles)[:, None, :]
    first = states[..., :half]
    second = states[..., half:]
    return jnp.concatenate(
        [first * cosine - second * sine, second * cosine + first * sine], axis=-1
    )


def smooth_from(input_peak, weight_peak):
    return jnp.sqrt(jnp.maximum(input_peak, 1e-05)) / jnp.sqrt(jnp.maximum(weight_peak, 1e-05))


def head_to_rows(matrix, tp_index, tp_count):
    sub_rows = matrix.shape[0] // tp_count
    columns = matrix.shape[1]
    whole = jnp.zeros((sub_rows, columns * tp_count), matrix.dtype)
    for shift in range(tp_count):
        target = lax.rem(tp_index + shift, tp_count)
        source = lax.rem(tp_index - shift + tp_count, tp_count)
        block = lax.dynamic_slice_in_dim(matrix, target * sub_rows, sub_rows)
        if shift > 0:
            pairs = [(i, (i + shift) % tp_count) for i in range(tp_count)]
            block = lax.ppermute(block, "tp", pairs)
        whole = lax.dynamic_update_slice_in_dim(whole, block, source * columns, axis=1)
    return whole


def on_device(hidden, norm_gain, w_query, w_key, w_value, doc_ids):
    tok_dev = hidden.shape[0]
    row_count = w_query.shape[0]
    tp_count = lax.axis_size("tp")
    tok_index = lax.axis_index("tok")
    tp_index = lax.axis_index("tp")
    heads_here = w_query.shape[1] // HEAD
    kv_here = w_key.shape[1] // HEAD
    group_size = QHEADS // KVH
    matrices = (w_query, w_key, w_value)
    states = hidden.astype(jnp.float32)
    normed = (
        states
        * lax.rsqrt(jnp.mean(states * states, axis=1, keepdims=True) + 1e-05)
        * norm_gain[None, :]
    ).astype(jnp.bfloat16)
    token_side = lax.all_to_all(normed, "tok", split_axis=1, concat_axis=0, tiled=True)
    input_rows = jnp.max(jnp.abs(token_side), axis=0).astype(jnp.float32)
    relaid = tuple(head_to_rows(matrix, tp_index, tp_count) for matrix in matrices)
    partial = jnp.dot(
        token_side, jnp.concatenate(matrices, axis=1), preferred_element_type=jnp.float32
    )
    summed = lax.psum_scatter(partial, "tok", scatter_dimension=0, tiled=True)
    query_columns, key_columns = w_query.shape[1], w_key.shape[1]
    projected = (
        summed[:, :query_columns],
        summed[:, query_columns : query_columns + key_columns],
        summed[:, query_columns + key_columns :],
    )
    local_peak = jnp.max(
        jnp.stack([jnp.max(jnp.abs(matrix), axis=1) for matrix in matrices]), axis=0
    ).astype(jnp.float32)
    row_peak = lax.pmax(local_peak, "tp")
    smoothing_rows = smooth_from(input_rows, row_peak)
    column_local = tuple(
        (
            jnp.max(jnp.abs(smoothing_rows[:, None] * matrix.astype(jnp.float32)), axis=0)
            for matrix in matrices
        )
    )
    column_global = lax.pmax(column_local, "tok")
    scales = tuple((jnp.maximum(column, 1e-05) / 127.0 for column in column_global))
    query_positions = tok_index * tok_dev + jnp.arange(tok_dev, dtype=jnp.int32)
    positions = query_positions.astype(jnp.float32)
    query = (
        rotate(projected[0].reshape(tok_dev, heads_here, HEAD), positions)
        .astype(jnp.bfloat16)
        .reshape(tok_dev, kv_here, group_size, HEAD)
    )
    key = (
        rotate(projected[1].reshape(tok_dev, kv_here, HEAD), positions)
        .astype(jnp.bfloat16)
        .reshape(tok_dev, kv_here * HEAD)
    )
    value = projected[2].astype(jnp.bfloat16)
    score_scale = 1.0 / math.sqrt(HEAD)
    highest = jnp.full((kv_here, group_size, tok_dev), -1e30, jnp.float32)
    key_block = lax.all_gather(key, "tok", axis=0, tiled=True)
    value_block = lax.all_gather(value, "tok", axis=0, tiled=True)
    doc_block = lax.all_gather(doc_ids, "tok", axis=0, tiled=True)
    length = key_block.shape[0]
    scores = (
        jnp.einsum(
            "tkgd,skd->kgts",
            query,
            key_block.reshape(length, kv_here, HEAD),
            preferred_element_type=jnp.float32,
        )
        * score_scale
    )
    key_positions = jnp.arange(length, dtype=jnp.int32)
    allowed = (doc_ids[:, None] == doc_block[None, :]) & (
        key_positions[None, :] <= query_positions[:, None]
    )
    scores = jnp.where(allowed, scores, -1e30)
    raised = jnp.maximum(highest, jnp.max(scores, axis=3))
    weights = jnp.where(allowed, jnp.exp(scores - raised[..., None]), 0.0)
    totals = jnp.sum(weights, axis=3)
    accumulated = jnp.einsum(
        "kgts,skd->kgtd",
        weights.astype(jnp.bfloat16),
        value_block.reshape(length, kv_here, HEAD),
        preferred_element_type=jnp.float32,
    )
    highest, totals, accumulated = (raised, totals, accumulated)
    attended = (
        (accumulated / totals[..., None])
        .transpose(2, 0, 1, 3)
        .reshape(tok_dev, heads_here * HEAD)
        .astype(jnp.bfloat16)
    )
    out_scale = lax.pmax(jnp.max(jnp.abs(attended), axis=0).astype(jnp.float32), "tok")
    sub_rows = row_count // tp_count
    smooth_part = lax.dynamic_slice_in_dim(smoothing_rows, tp_index * sub_rows, sub_rows)
    gain_part = lax.dynamic_slice_in_dim(
        norm_gain, tok_index * row_count + tp_index * sub_rows, sub_rows
    )
    folded_gain = gain_part / smooth_part
    every_scale = lax.all_gather(scales, "tp", axis=0, tiled=True)
    codes = tuple(
        (
            smooth_part[:, None] * block.astype(jnp.float32) / column_scale[None, :]
            for block, column_scale in zip(relaid, every_scale)
        )
    )
    return (
        attended,
        out_scale,
        folded_gain,
        codes[0],
        codes[1],
        codes[2],
        scales[0],
        scales[1],
        scales[2],
    )


def solution(mesh):
    in_specs = (P("tok", None), P(), P("tok", "tp"), P("tok", "tp"), P("tok", "tp"), P("tok"))
    out_specs = (
        P("tok", "tp"),
        P("tp"),
        P(("tok", "tp")),
        P(("tok", "tp"), None),
        P(("tok", "tp"), None),
        P(("tok", "tp"), None),
        P("tp"),
        P("tp"),
        P("tp"),
    )
    return jax.shard_map(
        on_device, mesh=mesh, in_specs=in_specs, out_specs=out_specs, check_vma=False
    )
```

```python
import functools
import math

import jax
import jax.numpy as jnp
from jax import lax
from jax.experimental import pallas as pl
from jax.experimental.pallas import tpu as pltpu
from jax.sharding import PartitionSpec as P

HEAD = 128
KVH = 8
QHEADS = 32


def rotate(states, positions):
    half = states.shape[-1] // 2
    inverse = jnp.exp(
        jnp.arange(half, dtype=jnp.float32) * (-2.0 * math.log(10000.0) / states.shape[-1])
    )
    angles = positions[:, None] * inverse[None, :]
    cosine = jnp.cos(angles)[:, None, :]
    sine = jnp.sin(angles)[:, None, :]
    first = states[..., :half]
    second = states[..., half:]
    return jnp.concatenate(
        [first * cosine - second * sine, second * cosine + first * sine], axis=-1
    )


def smooth_from(input_peak, weight_peak):
    return jnp.sqrt(jnp.maximum(input_peak, 1e-05)) / jnp.sqrt(jnp.maximum(weight_peak, 1e-05))


MESH = pl.DeviceIdType.MESH
QUAD = 4


def column_chunks(widths, most=512):
    return [
        (which, start, min(most, width - start))
        for which, width in enumerate(widths)
        for start in range(0, width, most)
    ]


def front_kernel(
    chunks,
    line,
    tp_count,
    normed_ref,
    wq_ref,
    wk_ref,
    wv_ref,
    sum_ref,
    peak_ref,
    rq_ref,
    rk_ref,
    rv_ref,
    held_q,
    held_k,
    held_v,
    tokens,
    partial,
    from_left,
    from_right,
    w_send,
    w_recv,
    t_send,
    t_recv,
    x_send,
    x_recv,
    x_local,
    r_send,
    r_recv,
    l_send,
    l_recv,
):
    me = lax.axis_index("tok")
    tp = lax.axis_index("tp")
    quad = lax.rem(me, QUAD)
    place = me // QUAD
    rows = wq_ref.shape[0]
    tok_dev = normed_ref.shape[0]
    sib = me + 1 - 2 * lax.rem(me, 2)
    side = me + 2 - 4 * (quad // 2)
    side_sib = side + 1 - 2 * lax.rem(me, 2)
    own = (wq_ref, wk_ref, wv_ref)
    held = (held_q, held_k, held_v)
    relaid = (rq_ref, rk_ref, rv_ref)
    sub = rows // tp_count

    def remote(src, dst, send, recv, tok, tp_to=None):
        return pltpu.make_async_remote_copy(
            src_ref=src,
            dst_ref=dst,
            send_sem=send,
            recv_sem=recv,
            device_id=(tok, tp if tp_to is None else tp_to),
            device_id_type=MESH,
        )

    barrier = pltpu.get_barrier_semaphore()
    pl.semaphore_signal(barrier, inc=1, device_id=(sib, tp), device_id_type=MESH)
    pl.semaphore_signal(barrier, inc=1, device_id=(side, tp), device_id_type=MESH)
    for step in range(1, line):
        other = lax.rem(place + step, line) * QUAD + quad
        pl.semaphore_signal(barrier, inc=1, device_id=(other, tp), device_id_type=MESH)
    for step in range(1, tp_count):
        other = lax.rem(tp + step, tp_count)
        pl.semaphore_signal(barrier, inc=1, device_id=(me, other), device_id_type=MESH)
    pl.semaphore_wait(barrier, 2 + (line - 1) + (tp_count - 1))

    def w_copy(kind, c):
        which, start, width = chunks[c]
        cols = pl.ds(start, width)
        if kind == 2:
            src = held[which].at[1, :, cols]
        else:
            src = own[which].at[:, cols]
        return remote(
            src,
            held[which].at[kind, :, cols],
            w_send.at[kind, c],
            w_recv.at[kind, c],
            side if kind == 1 else sib,
        )

    def t_copy(step):
        to = lax.rem(place + step, line)
        width = QUAD * rows
        return remote(
            normed_ref.at[:, pl.ds(pl.multiple_of(to * width, 128), width)],
            tokens.at[pl.ds(pl.multiple_of(place * tok_dev, 16), tok_dev)],
            t_send.at[step],
            t_recv.at[step],
            to * QUAD + quad,
        )

    def x_copy(which, step):
        to = lax.rem(tp + step, tp_count)
        width = own[which].shape[1]
        src = own[which].at[pl.ds(pl.multiple_of(to * sub, 16), sub)]
        dst = relaid[which].at[:, pl.ds(pl.multiple_of(tp * width, 128), width)]
        if step == 0:
            return pltpu.make_async_copy(src, dst, x_local.at[which])
        return remote(src, dst, x_send.at[which, step], x_recv.at[which, step], me, to)

    for step in range(1, line):
        t_copy(step).start()
    for c in range(len(chunks)):
        w_copy(1, c).start()
        w_copy(0, c).start()
    for which in range(3):
        for step in range(tp_count):
            x_copy(which, step).start()

    width = QUAD * rows
    tokens[pl.ds(pl.multiple_of(place * tok_dev, 16), tok_dev)] = normed_ref[
        :, pl.ds(pl.multiple_of(place * width, 128), width)
    ]
    for step in range(1, line):
        t_copy(step).wait_recv()
    peak_ref[...] = jnp.max(
        jnp.abs(tokens[...].astype(jnp.float32)), axis=0, keepdims=True
    )

    def span(c):
        which, start, size = chunks[c]
        base = sum(own[i].shape[1] for i in range(which)) + start
        return slice(base, base + size)

    def block(d):
        return pl.ds(pl.multiple_of(d * tok_dev, 8), tok_dev)

    def right(c, d):
        cols = span(c)
        return remote(
            partial.at[block(d), cols],
            from_left.at[block(d), cols],
            r_send.at[c, d],
            r_recv.at[c, d],
            me + QUAD,
        )

    def left(c, d):
        cols = span(c)
        return remote(
            partial.at[block(d), cols],
            from_right.at[block(d), cols],
            l_send.at[c, d],
            l_recv.at[c, d],
            me - QUAD,
        )

    def add_left(c, d):
        right(c, d).wait_recv()
        cols = span(c)
        partial[block(d), cols] = partial[block(d), cols] + from_left[block(d), cols]

    def add_right(c, d):
        left(c, d).wait_recv()
        cols = span(c)
        partial[block(d), cols] = partial[block(d), cols] + from_right[block(d), cols]

    def first_sends(c):
        @pl.when(place == 0)
        def _():
            def go(i, carry):
                right(c, line - 1 - i).start()
                return carry

            lax.fori_loop(0, line - 1, go, 0)

        @pl.when(place == line - 1)
        def _():
            def go(i, carry):
                left(c, i).start()
                return carry

            lax.fori_loop(0, line - 1, go, 0)

    def reduce(c):
        def go(i, carry):
            to_right = line - 1 - i

            @pl.when((place > 0) & (to_right > place))
            def _():
                add_left(c, to_right)
                right(c, to_right).start()

            @pl.when((place < line - 1) & (i < place))
            def _():
                add_right(c, i)
                left(c, i).start()

            return carry

        lax.fori_loop(0, line, go, 0)

        @pl.when(place > 0)
        def _():
            add_left(c, place)

        @pl.when(place < line - 1)
        def _():
            add_right(c, place)

        sum_ref[:, span(c)] = partial[block(place), span(c)]

    def columns_of(tok):
        return pl.ds(pl.multiple_of(lax.rem(tok, QUAD) * rows, 128), rows)

    for c in range(len(chunks)):
        which, start, size = chunks[c]
        cols = slice(start, start + size)
        w_copy(1, c).wait_recv()
        w_copy(2, c).start()
        total = jnp.dot(
            tokens[:, columns_of(me)],
            own[which][:, cols],
            preferred_element_type=jnp.float32,
        )
        total += jnp.dot(
            tokens[:, columns_of(side)],
            held[which][1, :, cols],
            preferred_element_type=jnp.float32,
        )
        w_copy(0, c).wait_recv()
        total += jnp.dot(
            tokens[:, columns_of(sib)],
            held[which][0, :, cols],
            preferred_element_type=jnp.float32,
        )
        w_copy(2, c).wait_recv()
        total += jnp.dot(
            tokens[:, columns_of(side_sib)],
            held[which][2, :, cols],
            preferred_element_type=jnp.float32,
        )
        partial[:, span(c)] = total
        first_sends(c)
        if c > 0:
            reduce(c - 1)
    reduce(len(chunks) - 1)

    for step in range(1, line):
        t_copy(step).wait_send()
    for c in range(len(chunks)):
        for kind in range(3):
            w_copy(kind, c).wait_send()

        def sent(d, carry):
            @pl.when(d > place)
            def _():
                right(c, d).wait_send()

            @pl.when(d < place)
            def _():
                left(c, d).wait_send()

            return carry

        lax.fori_loop(0, line, sent, 0)
    for which in range(3):
        x_copy(which, 0).wait()
        for step in range(1, tp_count):
            x_copy(which, step).wait_send()
            x_copy(which, step).wait_recv()


def front(normed, matrices):
    tok_count, tp_count = lax.axis_size("tok"), lax.axis_size("tp")
    line = tok_count // QUAD
    tok_dev = normed.shape[0]
    rows = matrices[0].shape[0]
    widths = [matrix.shape[1] for matrix in matrices]
    chunks = column_chunks(widths)
    total = sum(widths)
    vmem = pl.BlockSpec(memory_space=pltpu.VMEM)
    dma = pltpu.SemaphoreType.DMA
    return pl.pallas_call(
        functools.partial(front_kernel, chunks, line, tp_count),
        out_shape=(
            jax.ShapeDtypeStruct((tok_dev, total), jnp.float32),
            jax.ShapeDtypeStruct((1, QUAD * rows), jnp.float32),
        )
        + tuple(
            jax.ShapeDtypeStruct((rows // tp_count, width * tp_count), jnp.bfloat16)
            for width in widths
        ),
        in_specs=[vmem] * 4,
        out_specs=(vmem, vmem) + (pl.BlockSpec(memory_space=pl.ANY),) * 3,
        scratch_shapes=[
            pltpu.VMEM((3, rows, width), jnp.bfloat16) for width in widths
        ]
        + [
            pltpu.VMEM((line * tok_dev, QUAD * rows), jnp.bfloat16),
            pltpu.VMEM((line * tok_dev, total), jnp.float32),
            pltpu.VMEM((line * tok_dev, total), jnp.float32),
            pltpu.VMEM((line * tok_dev, total), jnp.float32),
            dma((3, len(chunks))),
            dma((3, len(chunks))),
            dma((line,)),
            dma((line,)),
            dma((3, tp_count)),
            dma((3, tp_count)),
            dma((3,)),
            dma((len(chunks), line)),
            dma((len(chunks), line)),
            dma((len(chunks), line)),
            dma((len(chunks), line)),
        ],
        compiler_params=pltpu.CompilerParams(
            collective_id=0, has_side_effects=True, vmem_limit_bytes=60 * 1024 * 1024
        ),
    )(normed, *matrices)


def on_device(hidden, norm_gain, w_query, w_key, w_value, doc_ids):
    tok_dev = hidden.shape[0]
    row_count = w_query.shape[0]
    tp_count = lax.axis_size("tp")
    tok_index = lax.axis_index("tok")
    tp_index = lax.axis_index("tp")
    heads_here = w_query.shape[1] // HEAD
    kv_here = w_key.shape[1] // HEAD
    group_size = QHEADS // KVH
    matrices = (w_query, w_key, w_value)
    states = hidden.astype(jnp.float32)
    normed = (
        states
        * lax.rsqrt(jnp.mean(states * states, axis=1, keepdims=True) + 1e-05)
        * norm_gain[None, :]
    ).astype(jnp.bfloat16)
    summed, peaks, *relaid = front(normed, matrices)
    query_columns, key_columns = w_query.shape[1], w_key.shape[1]
    projected = (
        summed[:, :query_columns],
        summed[:, query_columns : query_columns + key_columns],
        summed[:, query_columns + key_columns :],
    )
    tok_count = lax.axis_size("tok")
    quads = [[i + j for j in range(QUAD)] for i in range(0, tok_count, QUAD)]
    quad_peak = lax.pmax(peaks[0], "tok", axis_index_groups=quads)
    sub_rows = row_count // tp_count
    smooth_part = smooth_from(
        lax.dynamic_slice_in_dim(
            quad_peak, (tok_index % QUAD) * row_count + tp_index * sub_rows, sub_rows
        ),
        functools.reduce(
            jnp.maximum, [jnp.max(jnp.abs(block), axis=1) for block in relaid]
        ).astype(jnp.float32),
    )
    column_local = jnp.concatenate(
        [
            jnp.max(jnp.abs(smooth_part[:, None] * block.astype(jnp.float32)), axis=0)
            for block in relaid
        ]
    )
    every = jnp.maximum(lax.pmax(column_local, ("tok", "tp")), 1e-05) / 127.0
    every_scale = jnp.split(
        every, [relaid[0].shape[1], relaid[0].shape[1] + relaid[1].shape[1]]
    )
    scales = tuple(
        lax.dynamic_slice_in_dim(scale, tp_index * matrix.shape[1], matrix.shape[1])
        for scale, matrix in zip(every_scale, matrices)
    )
    query_positions = tok_index * tok_dev + jnp.arange(tok_dev, dtype=jnp.int32)
    positions = query_positions.astype(jnp.float32)
    query = (
        rotate(projected[0].reshape(tok_dev, heads_here, HEAD), positions)
        .astype(jnp.bfloat16)
        .reshape(tok_dev, kv_here, group_size, HEAD)
    )
    key = (
        rotate(projected[1].reshape(tok_dev, kv_here, HEAD), positions)
        .astype(jnp.bfloat16)
        .reshape(tok_dev, kv_here * HEAD)
    )
    value = projected[2].astype(jnp.bfloat16)
    score_scale = 1.0 / math.sqrt(HEAD)
    highest = jnp.full((kv_here, group_size, tok_dev), -1e30, jnp.float32)
    both = lax.all_gather(jnp.concatenate([key, value], axis=1), "tok", axis=0, tiled=True)
    key_block, value_block = both[:, :key_columns], both[:, key_columns:]
    doc_block = lax.all_gather(doc_ids, "tok", axis=0, tiled=True)
    length = key_block.shape[0]
    scores = (
        jnp.einsum(
            "tkgd,skd->kgts",
            query,
            key_block.reshape(length, kv_here, HEAD),
            preferred_element_type=jnp.float32,
        )
        * score_scale
    )
    key_positions = jnp.arange(length, dtype=jnp.int32)
    allowed = (doc_ids[:, None] == doc_block[None, :]) & (
        key_positions[None, :] <= query_positions[:, None]
    )
    scores = jnp.where(allowed, scores, -1e30)
    raised = jnp.maximum(highest, jnp.max(scores, axis=3))
    weights = jnp.where(allowed, jnp.exp(scores - raised[..., None]), 0.0)
    totals = jnp.sum(weights, axis=3)
    accumulated = jnp.einsum(
        "kgts,skd->kgtd",
        weights.astype(jnp.bfloat16),
        value_block.reshape(length, kv_here, HEAD),
        preferred_element_type=jnp.float32,
    )
    highest, totals, accumulated = (raised, totals, accumulated)
    attended = (
        (accumulated / totals[..., None])
        .transpose(2, 0, 1, 3)
        .reshape(tok_dev, heads_here * HEAD)
        .astype(jnp.bfloat16)
    )
    out_scale = lax.pmax(jnp.max(jnp.abs(attended), axis=0).astype(jnp.float32), "tok")
    gain_part = lax.dynamic_slice_in_dim(
        norm_gain, tok_index * row_count + tp_index * sub_rows, sub_rows
    )
    folded_gain = gain_part / smooth_part
    codes = tuple(
        (
            smooth_part[:, None] * block.astype(jnp.float32) / column_scale[None, :]
            for block, column_scale in zip(relaid, every_scale)
        )
    )
    return (
        attended,
        out_scale,
        folded_gain,
        codes[0],
        codes[1],
        codes[2],
        scales[0],
        scales[1],
        scales[2],
    )


def solution(mesh):
    in_specs = (P("tok", None), P(), P("tok", "tp"), P("tok", "tp"), P("tok", "tp"), P("tok"))
    out_specs = (
        P("tok", "tp"),
        P("tp"),
        P(("tok", "tp")),
        P(("tok", "tp"), None),
        P(("tok", "tp"), None),
        P(("tok", "tp"), None),
        P("tp"),
        P("tp"),
        P("tp"),
    )
    return jax.shard_map(
        on_device, mesh=mesh, in_specs=in_specs, out_specs=out_specs, check_vma=False
    )
```

```python
import functools
import math

import jax
import jax.numpy as jnp
from jax import lax
from jax.experimental import pallas as pl
from jax.experimental.pallas import tpu as pltpu
from jax.sharding import PartitionSpec as P

HEAD = 128
KVH = 8
QHEADS = 32


def rotate(states, positions):
    half = states.shape[-1] // 2
    inverse = jnp.exp(
        jnp.arange(half, dtype=jnp.float32) * (-2.0 * math.log(10000.0) / states.shape[-1])
    )
    angles = positions[:, None] * inverse[None, :]
    cosine = jnp.cos(angles)[:, None, :]
    sine = jnp.sin(angles)[:, None, :]
    first = states[..., :half]
    second = states[..., half:]
    return jnp.concatenate(
        [first * cosine - second * sine, second * cosine + first * sine], axis=-1
    )


def smooth_from(input_peak, weight_peak):
    return jnp.sqrt(jnp.maximum(input_peak, 1e-05)) / jnp.sqrt(jnp.maximum(weight_peak, 1e-05))


MESH = pl.DeviceIdType.MESH
QUAD = 4


def column_chunks(widths, most=512):
    return [
        (which, start, min(most, width - start))
        for which, width in enumerate(widths)
        for start in range(0, width, most)
    ]


def meet_all(barrier, me, tp, tok_count, tp_count):
    def greet(step, carry):
        other = lax.rem(me + step, tok_count)
        pl.semaphore_signal(barrier, inc=1, device_id=(other, tp), device_id_type=MESH)
        return carry

    lax.fori_loop(1, tok_count, greet, 0)
    for step in range(1, tp_count):
        other = lax.rem(tp + step, tp_count)
        pl.semaphore_signal(barrier, inc=1, device_id=(me, other), device_id_type=MESH)
    pl.semaphore_wait(barrier, tok_count - 1 + tp_count - 1)


def front_kernel(
    chunks,
    line,
    tp_count,
    normed_ref,
    doc_ref,
    wq_ref,
    wk_ref,
    wv_ref,
    sum_ref,
    peak_ref,
    docs_ref,
    rq_ref,
    rk_ref,
    rv_ref,
    mine,
    theirs,
    held_q,
    held_k,
    held_v,
    tokens,
    partial,
    from_left,
    from_right,
    w_send,
    w_recv,
    t_send,
    t_recv,
    x_send,
    x_recv,
    x_local,
    r_send,
    r_recv,
    l_send,
    l_recv,
    p_send,
    p_recv,
    d_send,
    d_recv,
):
    me = lax.axis_index("tok")
    tp = lax.axis_index("tp")
    quad = lax.rem(me, QUAD)
    place = me // QUAD
    rows = wq_ref.shape[0]
    tok_dev = normed_ref.shape[0]
    sib = me + 1 - 2 * lax.rem(me, 2)
    side = me + 2 - 4 * (quad // 2)
    side_sib = side + 1 - 2 * lax.rem(me, 2)
    own = (wq_ref, wk_ref, wv_ref)
    held = (held_q, held_k, held_v)
    relaid = (rq_ref, rk_ref, rv_ref)
    sub = rows // tp_count

    def remote(src, dst, send, recv, tok, tp_to=None):
        return pltpu.make_async_remote_copy(
            src_ref=src,
            dst_ref=dst,
            send_sem=send,
            recv_sem=recv,
            device_id=(tok, tp if tp_to is None else tp_to),
            device_id_type=MESH,
        )

    barrier = pltpu.get_barrier_semaphore()
    meet_all(barrier, me, tp, line * QUAD, tp_count)

    def w_copy(kind, c):
        which, start, width = chunks[c]
        cols = pl.ds(start, width)
        if kind == 2:
            src = held[which].at[1, :, cols]
        else:
            src = own[which].at[:, cols]
        return remote(
            src,
            held[which].at[kind, :, cols],
            w_send.at[kind, c],
            w_recv.at[kind, c],
            side if kind == 1 else sib,
        )

    def t_copy(step):
        to = lax.rem(place + step, line)
        width = QUAD * rows
        return remote(
            normed_ref.at[:, pl.ds(pl.multiple_of(to * width, 128), width)],
            tokens.at[pl.ds(pl.multiple_of(place * tok_dev, 16), tok_dev)],
            t_send.at[step],
            t_recv.at[step],
            to * QUAD + quad,
        )

    def x_copy(which, step):
        to = lax.rem(tp + step, tp_count)
        width = own[which].shape[1]
        src = own[which].at[pl.ds(pl.multiple_of(to * sub, 16), sub)]
        dst = relaid[which].at[:, pl.ds(pl.multiple_of(tp * width, 128), width)]
        if step == 0:
            return pltpu.make_async_copy(src, dst, x_local.at[which])
        return remote(src, dst, x_send.at[which, step], x_recv.at[which, step], me, to)

    def d_copy(step):
        return remote(
            doc_ref,
            docs_ref.at[me],
            d_send.at[step],
            d_recv.at[step],
            lax.rem(me + step, line * QUAD),
        )

    def p_copy(kind):
        return remote(
            mine,
            theirs.at[kind],
            p_send.at[kind],
            p_recv.at[kind],
            (sib, side, side_sib)[kind],
        )

    def d_start(step, carry):
        d_copy(step).start()
        return carry

    def d_wait(step, carry):
        d_copy(step).wait()
        return carry

    for step in range(1, line):
        t_copy(step).start()
    for c in range(len(chunks)):
        w_copy(1, c).start()
        w_copy(0, c).start()
    for which in range(3):
        for step in range(tp_count):
            x_copy(which, step).start()

    width = QUAD * rows
    tokens[pl.ds(pl.multiple_of(place * tok_dev, 16), tok_dev)] = normed_ref[
        :, pl.ds(pl.multiple_of(place * width, 128), width)
    ]
    for step in range(1, line):
        t_copy(step).wait_recv()
    mine[...] = jnp.max(
        jnp.abs(tokens[...].astype(jnp.float32)), axis=0, keepdims=True
    )
    docs_ref[me] = doc_ref[...]
    lax.fori_loop(1, line * QUAD, d_start, 0)

    def span(c):
        which, start, size = chunks[c]
        base = sum(own[i].shape[1] for i in range(which)) + start
        return slice(base, base + size)

    def block(d):
        return pl.ds(pl.multiple_of(d * tok_dev, 8), tok_dev)

    def right(c, d):
        cols = span(c)
        return remote(
            partial.at[block(d), cols],
            from_left.at[block(d), cols],
            r_send.at[c, d],
            r_recv.at[c, d],
            me + QUAD,
        )

    def left(c, d):
        cols = span(c)
        return remote(
            partial.at[block(d), cols],
            from_right.at[block(d), cols],
            l_send.at[c, d],
            l_recv.at[c, d],
            me - QUAD,
        )

    def add_left(c, d):
        right(c, d).wait_recv()
        cols = span(c)
        partial[block(d), cols] = partial[block(d), cols] + from_left[block(d), cols]

    def add_right(c, d):
        left(c, d).wait_recv()
        cols = span(c)
        partial[block(d), cols] = partial[block(d), cols] + from_right[block(d), cols]

    def first_sends(c):
        @pl.when(place == 0)
        def _():
            def go(i, carry):
                right(c, line - 1 - i).start()
                return carry

            lax.fori_loop(0, line - 1, go, 0)

        @pl.when(place == line - 1)
        def _():
            def go(i, carry):
                left(c, i).start()
                return carry

            lax.fori_loop(0, line - 1, go, 0)

    def reduce(c):
        def go(i, carry):
            to_right = line - 1 - i

            @pl.when((place > 0) & (to_right > place))
            def _():
                add_left(c, to_right)
                right(c, to_right).start()

            @pl.when((place < line - 1) & (i < place))
            def _():
                add_right(c, i)
                left(c, i).start()

            return carry

        lax.fori_loop(0, line, go, 0)

        @pl.when(place > 0)
        def _():
            add_left(c, place)

        @pl.when(place < line - 1)
        def _():
            add_right(c, place)

        sum_ref[:, span(c)] = partial[block(place), span(c)]

    def columns_of(tok):
        return pl.ds(pl.multiple_of(lax.rem(tok, QUAD) * rows, 128), rows)

    for c in range(len(chunks)):
        which, start, size = chunks[c]
        cols = slice(start, start + size)
        w_copy(1, c).wait_recv()
        w_copy(2, c).start()
        total = jnp.dot(
            tokens[:, columns_of(me)],
            own[which][:, cols],
            preferred_element_type=jnp.float32,
        )
        total += jnp.dot(
            tokens[:, columns_of(side)],
            held[which][1, :, cols],
            preferred_element_type=jnp.float32,
        )
        w_copy(0, c).wait_recv()
        total += jnp.dot(
            tokens[:, columns_of(sib)],
            held[which][0, :, cols],
            preferred_element_type=jnp.float32,
        )
        w_copy(2, c).wait_recv()
        total += jnp.dot(
            tokens[:, columns_of(side_sib)],
            held[which][2, :, cols],
            preferred_element_type=jnp.float32,
        )
        partial[:, span(c)] = total
        first_sends(c)
        if c == 0:
            for kind in range(3):
                p_copy(kind).start()
        if c > 0:
            reduce(c - 1)
    reduce(len(chunks) - 1)

    for kind in range(3):
        p_copy(kind).wait()
    peak_ref[...] = jnp.maximum(
        jnp.maximum(mine[...], theirs[0]), jnp.maximum(theirs[1], theirs[2])
    )
    lax.fori_loop(1, line * QUAD, d_wait, 0)
    for step in range(1, line):
        t_copy(step).wait_send()
    for c in range(len(chunks)):
        for kind in range(3):
            w_copy(kind, c).wait_send()

        def sent(d, carry):
            @pl.when(d > place)
            def _():
                right(c, d).wait_send()

            @pl.when(d < place)
            def _():
                left(c, d).wait_send()

            return carry

        lax.fori_loop(0, line, sent, 0)
    for which in range(3):
        x_copy(which, 0).wait()
        for step in range(1, tp_count):
            x_copy(which, step).wait_send()
            x_copy(which, step).wait_recv()


def front(normed, doc_row, matrices):
    tok_count, tp_count = lax.axis_size("tok"), lax.axis_size("tp")
    line = tok_count // QUAD
    tok_dev = normed.shape[0]
    rows = matrices[0].shape[0]
    widths = [matrix.shape[1] for matrix in matrices]
    chunks = column_chunks(widths)
    total = sum(widths)
    vmem = pl.BlockSpec(memory_space=pltpu.VMEM)
    dma = pltpu.SemaphoreType.DMA
    return pl.pallas_call(
        functools.partial(front_kernel, chunks, line, tp_count),
        out_shape=(
            jax.ShapeDtypeStruct((tok_dev, total), jnp.float32),
            jax.ShapeDtypeStruct((1, QUAD * rows), jnp.float32),
            jax.ShapeDtypeStruct((tok_count,) + doc_row.shape, jnp.int32),
        )
        + tuple(
            jax.ShapeDtypeStruct((rows // tp_count, width * tp_count), jnp.bfloat16)
            for width in widths
        ),
        in_specs=[vmem] * 5,
        out_specs=(vmem, vmem, vmem) + (pl.BlockSpec(memory_space=pl.ANY),) * 3,
        scratch_shapes=[
            pltpu.VMEM((1, QUAD * rows), jnp.float32),
            pltpu.VMEM((3, 1, QUAD * rows), jnp.float32),
        ]
        + [
            pltpu.VMEM((3, rows, width), jnp.bfloat16) for width in widths
        ]
        + [
            pltpu.VMEM((line * tok_dev, QUAD * rows), jnp.bfloat16),
            pltpu.VMEM((line * tok_dev, total), jnp.float32),
            pltpu.VMEM((line * tok_dev, total), jnp.float32),
            pltpu.VMEM((line * tok_dev, total), jnp.float32),
            dma((3, len(chunks))),
            dma((3, len(chunks))),
            dma((line,)),
            dma((line,)),
            dma((3, tp_count)),
            dma((3, tp_count)),
            dma((3,)),
            dma((len(chunks), line)),
            dma((len(chunks), line)),
            dma((len(chunks), line)),
            dma((len(chunks), line)),
            dma((3,)),
            dma((3,)),
            dma((tok_count,)),
            dma((tok_count,)),
        ],
        compiler_params=pltpu.CompilerParams(
            collective_id=0, has_side_effects=True, vmem_limit_bytes=60 * 1024 * 1024
        ),
    )(normed, doc_row, *matrices)


def back_kernel(
    line,
    tp_count,
    kv_here,
    query_ref,
    kv_ref,
    doc_mine_ref,
    doc_all_ref,
    column_ref,
    out_ref,
    out_peak_ref,
    scale_ref,
    cache,
    column_tp,
    column_mid,
    column_all,
    out_mine,
    out_all,
    z_send,
    z_recv,
    y_send,
    y_recv,
    s_send,
    s_recv,
    c_send,
    c_recv,
    a_send,
    a_recv,
    o_send,
    o_recv,
):
    me = lax.axis_index("tok")
    tp = lax.axis_index("tp")
    tok_count = line * QUAD
    quad = lax.rem(me, QUAD)
    place = me // QUAD
    tok_dev = query_ref.shape[0]
    keys = cache.shape[0]
    sib = me + 1 - 2 * lax.rem(me, 2)
    side = me + 2 - 4 * (quad // 2)

    def remote(src, dst, send, recv, tok, tp_to=None):
        return pltpu.make_async_remote_copy(
            src_ref=src,
            dst_ref=dst,
            send_sem=send,
            recv_sem=recv,
            device_id=(tok, tp if tp_to is None else tp_to),
            device_id_type=MESH,
        )

    def rows_of(tok):
        return pl.ds(pl.multiple_of(tok * tok_dev, 16), tok_dev)

    def z_copy(step):
        to = lax.rem(place + step, line) * QUAD + quad
        return remote(
            kv_ref, cache.at[rows_of(me)], z_send.at[step], z_recv.at[step], to
        )

    def line_source(step):
        return lax.rem(place - step + line, line) * QUAD

    def y_copy(step):
        tok = line_source(step) + quad
        src = kv_ref if step == 0 else cache.at[rows_of(tok)]
        return remote(
            src, cache.at[rows_of(tok)], y_send.at[step], y_recv.at[step], side
        )

    def s_copy(step, of_side):
        tok = line_source(step) + (lax.rem(side, QUAD) if of_side else quad)
        src = kv_ref if step == 0 and not of_side else cache.at[rows_of(tok)]
        slot = step + (line if of_side else 0)
        return remote(src, cache.at[rows_of(tok)], s_send.at[slot], s_recv.at[slot], sib)

    def c_copy(step):
        return remote(
            column_ref,
            column_tp.at[step],
            c_send.at[step],
            c_recv.at[step],
            me,
            lax.rem(tp + step, tp_count),
        )

    def a_copy(step):
        return remote(
            column_mid,
            column_all.at[me],
            a_send.at[step],
            a_recv.at[step],
            lax.rem(me + step, tok_count),
        )

    def o_copy(step):
        return remote(
            out_mine,
            out_all.at[me],
            o_send.at[step],
            o_recv.at[step],
            lax.rem(me + step, tok_count),
        )

    def each(copy, act):
        def go(step, carry):
            getattr(copy(step), act)()
            return carry

        lax.fori_loop(1, tok_count, go, 0)

    meet_all(pltpu.get_barrier_semaphore(), me, tp, tok_count, tp_count)
    for step in range(1, tp_count):
        c_copy(step).start()
    y_copy(0).start()
    for step in range(1, line):
        z_copy(step).start()
    s_copy(0, False).start()
    cache[rows_of(me)] = kv_ref[...]
    joined = column_ref[...]
    for step in range(1, tp_count):
        c_copy(step).wait()
        joined = jnp.maximum(joined, column_tp[step])
    column_mid[...] = joined
    column_all[me] = joined
    for step in range(1, line):
        z_copy(step).wait_recv()
        y_copy(step).start()
        s_copy(step, False).start()
    each(a_copy, "start")
    for step in range(line):
        y_copy(step).wait_recv()
        s_copy(step, True).start()
    for step in range(line):
        s_copy(step, False).wait_recv()
        s_copy(step, True).wait_recv()

    position = lax.broadcasted_iota(jnp.int32, (tok_dev, keys), 0) + me * tok_dev
    allowed = (doc_mine_ref[...] == doc_all_ref[...]) & (
        lax.broadcasted_iota(jnp.int32, (tok_dev, keys), 1) <= position
    )
    group = QHEADS // KVH
    for kv in range(kv_here):
        heads = [
            slice((kv * group + g) * HEAD, (kv * group + g + 1) * HEAD)
            for g in range(group)
        ]
        query = jnp.concatenate([query_ref[:, head] for head in heads], axis=0)
        key = cache[:, kv * HEAD : (kv + 1) * HEAD]
        value = cache[:, (kv_here + kv) * HEAD : (kv_here + kv + 1) * HEAD]
        scores = lax.dot_general(
            query, key, (((1,), (1,)), ((), ())), preferred_element_type=jnp.float32
        ) * (1.0 / math.sqrt(HEAD))
        scores = jnp.where(
            allowed[None], scores.reshape(group, tok_dev, keys), -1e30
        ).reshape(group * tok_dev, keys)
        weights = jnp.exp(scores - jnp.max(scores, axis=1, keepdims=True))
        totals = jnp.sum(weights, axis=1, keepdims=True)
        mixed = jnp.dot(
            weights.astype(jnp.bfloat16), value, preferred_element_type=jnp.float32
        )
        mixed = (mixed / totals).astype(jnp.bfloat16)
        for g, head in enumerate(heads):
            piece = mixed[g * tok_dev : (g + 1) * tok_dev]
            out_ref[:, head] = piece
            out_mine[:, head] = jnp.max(
                jnp.abs(piece.astype(jnp.float32)), axis=0, keepdims=True
            )
    out_all[me] = out_mine[...]
    each(o_copy, "start")
    each(a_copy, "wait")
    scale_ref[...] = jnp.maximum(jnp.max(column_all[...], axis=0), 1e-05) / 127.0
    each(o_copy, "wait")
    out_peak_ref[...] = jnp.max(out_all[...], axis=0)
    for step in range(line):
        if step > 0:
            z_copy(step).wait_send()
        y_copy(step).wait_send()
        s_copy(step, False).wait_send()
        s_copy(step, True).wait_send()


def back(query, keys_values, doc_mine, doc_all, column_local):
    tok_count, tp_count = lax.axis_size("tok"), lax.axis_size("tp")
    line = tok_count // QUAD
    tok_dev, width = query.shape
    kv_here = keys_values.shape[1] // (2 * HEAD)
    columns = column_local.shape[1]
    vmem = pl.BlockSpec(memory_space=pltpu.VMEM)
    dma = pltpu.SemaphoreType.DMA
    f32 = jnp.float32
    return pl.pallas_call(
        functools.partial(back_kernel, line, tp_count, kv_here),
        out_shape=(
            jax.ShapeDtypeStruct((tok_dev, width), jnp.bfloat16),
            jax.ShapeDtypeStruct((1, width), f32),
            jax.ShapeDtypeStruct((1, columns), f32),
        ),
        in_specs=[vmem] * 5,
        out_specs=(vmem,) * 3,
        scratch_shapes=[
            pltpu.VMEM((tok_dev * tok_count, keys_values.shape[1]), jnp.bfloat16),
            pltpu.VMEM((tp_count, 1, columns), f32),
            pltpu.VMEM((1, columns), f32),
            pltpu.VMEM((tok_count, 1, columns), f32),
            pltpu.VMEM((1, width), f32),
            pltpu.VMEM((tok_count, 1, width), f32),
        ]
        + [dma((line,))] * 4
        + [dma((2 * line,))] * 2
        + [dma((tp_count,))] * 2
        + [dma((tok_count,))] * 4,
        compiler_params=pltpu.CompilerParams(
            collective_id=1, has_side_effects=True, vmem_limit_bytes=60 * 1024 * 1024
        ),
    )(query, keys_values, doc_mine, doc_all, column_local)


def on_device(hidden, norm_gain, w_query, w_key, w_value, doc_ids):
    tok_dev = hidden.shape[0]
    row_count = w_query.shape[0]
    tp_count = lax.axis_size("tp")
    tok_index = lax.axis_index("tok")
    tp_index = lax.axis_index("tp")
    heads_here = w_query.shape[1] // HEAD
    kv_here = w_key.shape[1] // HEAD
    matrices = (w_query, w_key, w_value)
    states = hidden.astype(jnp.float32)
    normed = (
        states
        * lax.rsqrt(jnp.mean(states * states, axis=1, keepdims=True) + 1e-05)
        * norm_gain[None, :]
    ).astype(jnp.bfloat16)
    lanes = -tok_dev % 128
    doc_row = jnp.pad(doc_ids, (0, lanes))[None]
    summed, peaks, docs, *relaid = front(normed, doc_row, matrices)
    doc_all = docs[:, 0, :tok_dev].reshape(1, -1)
    query_columns, key_columns = w_query.shape[1], w_key.shape[1]
    projected = (
        summed[:, :query_columns],
        summed[:, query_columns : query_columns + key_columns],
        summed[:, query_columns + key_columns :],
    )
    sub_rows = row_count // tp_count
    smooth_part = smooth_from(
        lax.dynamic_slice_in_dim(
            peaks[0], (tok_index % QUAD) * row_count + tp_index * sub_rows, sub_rows
        ),
        functools.reduce(
            jnp.maximum, [jnp.max(jnp.abs(block), axis=1) for block in relaid]
        ).astype(jnp.float32),
    )
    column_local = jnp.concatenate(
        [
            jnp.max(jnp.abs(smooth_part[:, None] * block.astype(jnp.float32)), axis=0)
            for block in relaid
        ]
    )
    query_positions = tok_index * tok_dev + jnp.arange(tok_dev, dtype=jnp.int32)
    positions = query_positions.astype(jnp.float32)
    query = (
        rotate(projected[0].reshape(tok_dev, heads_here, HEAD), positions)
        .astype(jnp.bfloat16)
        .reshape(tok_dev, heads_here * HEAD)
    )
    key = (
        rotate(projected[1].reshape(tok_dev, kv_here, HEAD), positions)
        .astype(jnp.bfloat16)
        .reshape(tok_dev, kv_here * HEAD)
    )
    value = projected[2].astype(jnp.bfloat16)
    attended, out_scale, column_scales = back(
        query,
        jnp.concatenate([key, value], axis=1),
        doc_ids[:, None],
        doc_all,
        column_local[None],
    )
    out_scale = out_scale[0]
    every = column_scales[0]
    every_scale = jnp.split(
        every, [relaid[0].shape[1], relaid[0].shape[1] + relaid[1].shape[1]]
    )
    scales = tuple(
        lax.dynamic_slice_in_dim(scale, tp_index * matrix.shape[1], matrix.shape[1])
        for scale, matrix in zip(every_scale, matrices)
    )
    gain_part = lax.dynamic_slice_in_dim(
        norm_gain, tok_index * row_count + tp_index * sub_rows, sub_rows
    )
    folded_gain = gain_part / smooth_part
    codes = tuple(
        (
            smooth_part[:, None] * block.astype(jnp.float32) / column_scale[None, :]
            for block, column_scale in zip(relaid, every_scale)
        )
    )
    return (
        attended,
        out_scale,
        folded_gain,
        codes[0],
        codes[1],
        codes[2],
        scales[0],
        scales[1],
        scales[2],
    )


def solution(mesh):
    in_specs = (P("tok", None), P(), P("tok", "tp"), P("tok", "tp"), P("tok", "tp"), P("tok"))
    out_specs = (
        P("tok", "tp"),
        P("tp"),
        P(("tok", "tp")),
        P(("tok", "tp"), None),
        P(("tok", "tp"), None),
        P(("tok", "tp"), None),
        P("tp"),
        P("tp"),
        P("tp"),
    )
    return jax.shard_map(
        on_device, mesh=mesh, in_specs=in_specs, out_specs=out_specs, check_vma=False
    )
```

```python
import functools
import math

import jax
import jax.numpy as jnp
from jax import lax
from jax.experimental import pallas as pl
from jax.experimental.pallas import tpu as pltpu
from jax.sharding import PartitionSpec as P

HEAD = 128
KVH = 8
QHEADS = 32


def rotation(positions):
    half = HEAD // 2
    inverse = jnp.exp(
        jnp.arange(half, dtype=jnp.float32) * (-2.0 * math.log(10000.0) / HEAD)
    )
    angles = positions[:, None] * inverse[None, :]
    cosine, sine = jnp.cos(angles), jnp.sin(angles)
    return (
        jnp.concatenate([cosine, cosine], axis=1),
        jnp.concatenate([-sine, sine], axis=1),
    )


def smooth_from(input_peak, weight_peak):
    return jnp.sqrt(jnp.maximum(input_peak, 1e-05)) / jnp.sqrt(jnp.maximum(weight_peak, 1e-05))


MESH = pl.DeviceIdType.MESH
QUAD = 4


def column_chunks(widths, most=512):
    return [
        (which, start, min(most, width - start))
        for which, width in enumerate(widths)
        for start in range(0, width, most)
    ]


def meet_all(barrier, me, tp, tok_count, tp_count):
    def greet(step, carry):
        other = lax.rem(me + step, tok_count)
        pl.semaphore_signal(barrier, inc=1, device_id=(other, tp), device_id_type=MESH)
        return carry

    lax.fori_loop(1, tok_count, greet, 0)
    for step in range(1, tp_count):
        other = lax.rem(tp + step, tp_count)
        pl.semaphore_signal(barrier, inc=1, device_id=(me, other), device_id_type=MESH)
    pl.semaphore_wait(barrier, tok_count - 1 + tp_count - 1)


def front_kernel(
    chunks,
    line,
    tp_count,
    share,
    normed_ref,
    doc_ref,
    cosine_ref,
    sine_ref,
    wq_ref,
    wk_ref,
    wv_ref,
    query_ref,
    kv_ref,
    peak_ref,
    docs_ref,
    rq_ref,
    rk_ref,
    rv_ref,
    mine,
    theirs,
    held_q,
    held_k,
    held_v,
    tokens,
    partial,
    from_left,
    from_right,
    w_send,
    w_recv,
    t_send,
    t_recv,
    m_send,
    m_recv,
    x_send,
    x_recv,
    x_local,
    r_send,
    r_recv,
    l_send,
    l_recv,
    p_send,
    p_recv,
    d_send,
    d_recv,
):
    me = lax.axis_index("tok")
    tp = lax.axis_index("tp")
    quad = lax.rem(me, QUAD)
    place = me // QUAD
    rows = wq_ref.shape[0]
    tok_dev = normed_ref.shape[0]
    sib = me + 1 - 2 * lax.rem(me, 2)
    side = me + 2 - 4 * (quad // 2)
    side_sib = side + 1 - 2 * lax.rem(me, 2)
    own = (wq_ref, wk_ref, wv_ref)
    held = (held_q, held_k, held_v)
    relaid = (rq_ref, rk_ref, rv_ref)
    sub = rows // tp_count

    def remote(src, dst, send, recv, tok, tp_to=None):
        return pltpu.make_async_remote_copy(
            src_ref=src,
            dst_ref=dst,
            send_sem=send,
            recv_sem=recv,
            device_id=(tok, tp if tp_to is None else tp_to),
            device_id_type=MESH,
        )

    barrier = pltpu.get_barrier_semaphore()
    meet_all(barrier, me, tp, line * QUAD, tp_count)

    def w_copy(kind, c):
        which, start, width = chunks[c]
        cols = pl.ds(start, width)
        if kind == 2:
            src = held[which].at[1, :, cols]
        else:
            src = own[which].at[:, cols]
        return remote(
            src,
            held[which].at[kind, :, cols],
            w_send.at[kind, c],
            w_recv.at[kind, c],
            side if kind == 1 else sib,
        )

    part = tok_dev // share
    piece = lax.rem(tp, share)
    mate = tp + 1 - 2 * piece

    def t_copy(step):
        to = lax.rem(place + step, line)
        width = QUAD * rows
        first = pl.multiple_of(piece * part, 16)
        return remote(
            normed_ref.at[
                pl.ds(first, part), pl.ds(pl.multiple_of(to * width, 128), width)
            ],
            tokens.at[pl.ds(pl.multiple_of(place * tok_dev + first, 16), part)],
            t_send.at[step],
            t_recv.at[step],
            to * QUAD + quad,
        )

    def m_copy(step):
        source = lax.rem(place - step + line, line)
        first = pl.multiple_of(source * tok_dev + piece * part, 16)
        got = tokens.at[pl.ds(first, part)]
        return remote(got, got, m_send.at[step], m_recv.at[step], me, mate)

    def x_copy(which, step):
        to = lax.rem(tp + step, tp_count)
        width = own[which].shape[1]
        src = own[which].at[pl.ds(pl.multiple_of(to * sub, 16), sub)]
        dst = relaid[which].at[:, pl.ds(pl.multiple_of(tp * width, 128), width)]
        if step == 0:
            return pltpu.make_async_copy(src, dst, x_local.at[which])
        return remote(src, dst, x_send.at[which, step], x_recv.at[which, step], me, to)

    def d_copy(step):
        return remote(
            doc_ref,
            docs_ref.at[me],
            d_send.at[step],
            d_recv.at[step],
            lax.rem(me + step, line * QUAD),
        )

    def p_copy(kind):
        return remote(
            mine,
            theirs.at[kind],
            p_send.at[kind],
            p_recv.at[kind],
            (sib, side, side_sib)[kind],
        )

    def d_start(step, carry):
        d_copy(step).start()
        return carry

    def d_wait(step, carry):
        d_copy(step).wait()
        return carry

    for step in range(1, line):
        t_copy(step).start()
    for c in range(len(chunks)):
        w_copy(1, c).start()
        w_copy(0, c).start()
    width = QUAD * rows
    tokens[pl.ds(pl.multiple_of(place * tok_dev, 16), tok_dev)] = normed_ref[
        :, pl.ds(pl.multiple_of(place * width, 128), width)
    ]
    for step in range(1, line):
        t_copy(step).wait_recv()
        if share == 2:
            m_copy(step).start()
    for which in range(3):
        for step in range(tp_count):
            x_copy(which, step).start()
    if share == 2:
        for step in range(1, line):
            m_copy(step).wait_recv()
    mine[...] = jnp.max(
        jnp.abs(tokens[...].astype(jnp.float32)), axis=0, keepdims=True
    )
    docs_ref[me] = doc_ref[...]
    lax.fori_loop(1, line * QUAD, d_start, 0)

    def span(c):
        which, start, size = chunks[c]
        base = sum(own[i].shape[1] for i in range(which)) + start
        return slice(base, base + size)

    def block(d):
        return pl.ds(pl.multiple_of(d * tok_dev, 8), tok_dev)

    def right(c, d):
        cols = span(c)
        return remote(
            partial.at[block(d), cols],
            from_left.at[block(d), cols],
            r_send.at[c, d],
            r_recv.at[c, d],
            me + QUAD,
        )

    def left(c, d):
        cols = span(c)
        return remote(
            partial.at[block(d), cols],
            from_right.at[block(d), cols],
            l_send.at[c, d],
            l_recv.at[c, d],
            me - QUAD,
        )

    def add_left(c, d):
        right(c, d).wait_recv()
        cols = span(c)
        partial[block(d), cols] = partial[block(d), cols] + from_left[block(d), cols]

    def add_right(c, d):
        left(c, d).wait_recv()
        cols = span(c)
        partial[block(d), cols] = partial[block(d), cols] + from_right[block(d), cols]

    def first_sends(c):
        @pl.when(place == 0)
        def _():
            def go(i, carry):
                right(c, line - 1 - i).start()
                return carry

            lax.fori_loop(0, line - 1, go, 0)

        @pl.when(place == line - 1)
        def _():
            def go(i, carry):
                left(c, i).start()
                return carry

            lax.fori_loop(0, line - 1, go, 0)

    def reduce(c):
        def go(i, carry):
            to_right = line - 1 - i

            @pl.when((place > 0) & (to_right > place))
            def _():
                add_left(c, to_right)
                right(c, to_right).start()

            @pl.when((place < line - 1) & (i < place))
            def _():
                add_right(c, i)
                left(c, i).start()

            return carry

        lax.fori_loop(0, line, go, 0)

    def finish(c):
        @pl.when(place > 0)
        def _():
            add_left(c, place)

        @pl.when(place < line - 1)
        def _():
            add_right(c, place)

        which, start, size = chunks[c]
        for head in range(size // HEAD):
            base = span(c).start + head * HEAD
            states = partial[block(place), base : base + HEAD]
            if which < 2:
                states = (
                    states * cosine_ref[...]
                    + pltpu.roll(states, HEAD // 2, 1) * sine_ref[...]
                )
            at = start + head * HEAD + (wk_ref.shape[1] if which == 2 else 0)
            target = query_ref if which == 0 else kv_ref
            target[:, at : at + HEAD] = states.astype(jnp.bfloat16)

    def columns_of(tok):
        return pl.ds(pl.multiple_of(lax.rem(tok, QUAD) * rows, 128), rows)

    for c in range(len(chunks)):
        which, start, size = chunks[c]
        cols = slice(start, start + size)
        w_copy(1, c).wait_recv()
        w_copy(2, c).start()
        total = jnp.dot(
            tokens[:, columns_of(me)],
            own[which][:, cols],
            preferred_element_type=jnp.float32,
        )
        total += jnp.dot(
            tokens[:, columns_of(side)],
            held[which][1, :, cols],
            preferred_element_type=jnp.float32,
        )
        w_copy(0, c).wait_recv()
        total += jnp.dot(
            tokens[:, columns_of(sib)],
            held[which][0, :, cols],
            preferred_element_type=jnp.float32,
        )
        w_copy(2, c).wait_recv()
        total += jnp.dot(
            tokens[:, columns_of(side_sib)],
            held[which][2, :, cols],
            preferred_element_type=jnp.float32,
        )
        partial[:, span(c)] = total
        first_sends(c)
        if c == 0:
            for kind in range(3):
                p_copy(kind).start()
        if c > 0:
            reduce(c - 1)
    reduce(len(chunks) - 1)
    for c in range(len(chunks)):
        finish(c)

    for kind in range(3):
        p_copy(kind).wait()
    peak_ref[...] = jnp.maximum(
        jnp.maximum(mine[...], theirs[0]), jnp.maximum(theirs[1], theirs[2])
    )
    lax.fori_loop(1, line * QUAD, d_wait, 0)
    for step in range(1, line):
        t_copy(step).wait_send()
        if share == 2:
            m_copy(step).wait_send()
    for c in range(len(chunks)):
        for kind in range(3):
            w_copy(kind, c).wait_send()

        def sent(d, carry):
            @pl.when(d > place)
            def _():
                right(c, d).wait_send()

            @pl.when(d < place)
            def _():
                left(c, d).wait_send()

            return carry

        lax.fori_loop(0, line, sent, 0)
    for which in range(3):
        x_copy(which, 0).wait()
        for step in range(1, tp_count):
            x_copy(which, step).wait_send()
            x_copy(which, step).wait_recv()


def front(normed, doc_row, cosine, sine, matrices):
    tok_count, tp_count = lax.axis_size("tok"), lax.axis_size("tp")
    line = tok_count // QUAD
    tok_dev = normed.shape[0]
    rows = matrices[0].shape[0]
    widths = [matrix.shape[1] for matrix in matrices]
    chunks = column_chunks(widths)
    total = sum(widths)
    share = 2 if tp_count % 2 == 0 and tok_dev % 32 == 0 else 1
    vmem = pl.BlockSpec(memory_space=pltpu.VMEM)
    dma = pltpu.SemaphoreType.DMA
    return pl.pallas_call(
        functools.partial(front_kernel, chunks, line, tp_count, share),
        out_shape=(
            jax.ShapeDtypeStruct((tok_dev, widths[0]), jnp.bfloat16),
            jax.ShapeDtypeStruct((tok_dev, widths[1] + widths[2]), jnp.bfloat16),
            jax.ShapeDtypeStruct((1, QUAD * rows), jnp.float32),
            jax.ShapeDtypeStruct((tok_count,) + doc_row.shape, jnp.int32),
        )
        + tuple(
            jax.ShapeDtypeStruct((rows // tp_count, width * tp_count), jnp.bfloat16)
            for width in widths
        ),
        in_specs=[vmem] * 7,
        out_specs=(vmem,) * 4 + (pl.BlockSpec(memory_space=pl.ANY),) * 3,
        scratch_shapes=[
            pltpu.VMEM((1, QUAD * rows), jnp.float32),
            pltpu.VMEM((3, 1, QUAD * rows), jnp.float32),
        ]
        + [
            pltpu.VMEM((3, rows, width), jnp.bfloat16) for width in widths
        ]
        + [
            pltpu.VMEM((line * tok_dev, QUAD * rows), jnp.bfloat16),
            pltpu.VMEM((line * tok_dev, total), jnp.float32),
            pltpu.VMEM((line * tok_dev, total), jnp.float32),
            pltpu.VMEM((line * tok_dev, total), jnp.float32),
            dma((3, len(chunks))),
            dma((3, len(chunks))),
            dma((line,)),
            dma((line,)),
            dma((line,)),
            dma((line,)),
            dma((3, tp_count)),
            dma((3, tp_count)),
            dma((3,)),
            dma((len(chunks), line)),
            dma((len(chunks), line)),
            dma((len(chunks), line)),
            dma((len(chunks), line)),
            dma((3,)),
            dma((3,)),
            dma((tok_count,)),
            dma((tok_count,)),
        ],
        compiler_params=pltpu.CompilerParams(
            collective_id=0, has_side_effects=True, vmem_limit_bytes=60 * 1024 * 1024
        ),
    )(normed, doc_row, cosine, sine, *matrices)


def back_kernel(
    line,
    tp_count,
    kv_here,
    query_ref,
    kv_ref,
    doc_mine_ref,
    doc_all_ref,
    column_ref,
    out_ref,
    out_peak_ref,
    scale_ref,
    cache,
    column_tp,
    column_mid,
    column_all,
    out_mine,
    out_all,
    z_send,
    z_recv,
    y_send,
    y_recv,
    s_send,
    s_recv,
    c_send,
    c_recv,
    a_send,
    a_recv,
    o_send,
    o_recv,
):
    me = lax.axis_index("tok")
    tp = lax.axis_index("tp")
    tok_count = line * QUAD
    quad = lax.rem(me, QUAD)
    place = me // QUAD
    tok_dev = query_ref.shape[0]
    keys = cache.shape[0]
    sib = me + 1 - 2 * lax.rem(me, 2)
    side = me + 2 - 4 * (quad // 2)

    def remote(src, dst, send, recv, tok, tp_to=None):
        return pltpu.make_async_remote_copy(
            src_ref=src,
            dst_ref=dst,
            send_sem=send,
            recv_sem=recv,
            device_id=(tok, tp if tp_to is None else tp_to),
            device_id_type=MESH,
        )

    def rows_of(tok):
        return pl.ds(pl.multiple_of(tok * tok_dev, 16), tok_dev)

    def z_copy(step):
        to = lax.rem(place + step, line) * QUAD + quad
        return remote(
            kv_ref, cache.at[rows_of(me)], z_send.at[step], z_recv.at[step], to
        )

    def line_source(step):
        return lax.rem(place - step + line, line) * QUAD

    def y_copy(step):
        tok = line_source(step) + quad
        src = kv_ref if step == 0 else cache.at[rows_of(tok)]
        return remote(
            src, cache.at[rows_of(tok)], y_send.at[step], y_recv.at[step], side
        )

    def s_copy(step, of_side):
        tok = line_source(step) + (lax.rem(side, QUAD) if of_side else quad)
        src = kv_ref if step == 0 and not of_side else cache.at[rows_of(tok)]
        slot = step + (line if of_side else 0)
        return remote(src, cache.at[rows_of(tok)], s_send.at[slot], s_recv.at[slot], sib)

    def c_copy(step):
        return remote(
            column_ref,
            column_tp.at[step],
            c_send.at[step],
            c_recv.at[step],
            me,
            lax.rem(tp + step, tp_count),
        )

    def a_copy(step):
        return remote(
            column_mid,
            column_all.at[me],
            a_send.at[step],
            a_recv.at[step],
            lax.rem(me + step, tok_count),
        )

    def o_copy(step):
        return remote(
            out_mine,
            out_all.at[me],
            o_send.at[step],
            o_recv.at[step],
            lax.rem(me + step, tok_count),
        )

    def each(copy, act):
        def go(step, carry):
            getattr(copy(step), act)()
            return carry

        lax.fori_loop(1, tok_count, go, 0)

    meet_all(pltpu.get_barrier_semaphore(), me, tp, tok_count, tp_count)
    for step in range(1, tp_count):
        c_copy(step).start()
    y_copy(0).start()
    for step in range(1, line):
        z_copy(step).start()
    s_copy(0, False).start()
    cache[rows_of(me)] = kv_ref[...]
    joined = column_ref[...]
    for step in range(1, tp_count):
        c_copy(step).wait()
        joined = jnp.maximum(joined, column_tp[step])
    column_mid[...] = joined
    column_all[me] = joined
    for step in range(1, line):
        z_copy(step).wait_recv()
        y_copy(step).start()
        s_copy(step, False).start()
    each(a_copy, "start")
    for step in range(line):
        y_copy(step).wait_recv()
        s_copy(step, True).start()
    for step in range(line):
        s_copy(step, False).wait_recv()
        s_copy(step, True).wait_recv()

    position = lax.broadcasted_iota(jnp.int32, (tok_dev, keys), 0) + me * tok_dev
    allowed = (doc_mine_ref[...] == doc_all_ref[...]) & (
        lax.broadcasted_iota(jnp.int32, (tok_dev, keys), 1) <= position
    )
    group = QHEADS // KVH
    for kv in range(kv_here):
        heads = [
            slice((kv * group + g) * HEAD, (kv * group + g + 1) * HEAD)
            for g in range(group)
        ]
        query = jnp.concatenate([query_ref[:, head] for head in heads], axis=0)
        key = cache[:, kv * HEAD : (kv + 1) * HEAD]
        value = cache[:, (kv_here + kv) * HEAD : (kv_here + kv + 1) * HEAD]
        scores = lax.dot_general(
            query, key, (((1,), (1,)), ((), ())), preferred_element_type=jnp.float32
        ) * (1.0 / math.sqrt(HEAD))
        scores = jnp.where(
            allowed[None], scores.reshape(group, tok_dev, keys), -1e30
        ).reshape(group * tok_dev, keys)
        weights = jnp.exp(scores - jnp.max(scores, axis=1, keepdims=True))
        totals = jnp.sum(weights, axis=1, keepdims=True)
        mixed = jnp.dot(
            weights.astype(jnp.bfloat16), value, preferred_element_type=jnp.float32
        )
        mixed = (mixed / totals).astype(jnp.bfloat16)
        for g, head in enumerate(heads):
            piece = mixed[g * tok_dev : (g + 1) * tok_dev]
            out_ref[:, head] = piece
            out_mine[:, head] = jnp.max(
                jnp.abs(piece.astype(jnp.float32)), axis=0, keepdims=True
            )
    out_all[me] = out_mine[...]
    each(o_copy, "start")
    each(a_copy, "wait")
    scale_ref[...] = jnp.maximum(jnp.max(column_all[...], axis=0), 1e-05) / 127.0
    each(o_copy, "wait")
    out_peak_ref[...] = jnp.max(out_all[...], axis=0)
    for step in range(line):
        if step > 0:
            z_copy(step).wait_send()
        y_copy(step).wait_send()
        s_copy(step, False).wait_send()
        s_copy(step, True).wait_send()


def back(query, keys_values, doc_mine, doc_all, column_local):
    tok_count, tp_count = lax.axis_size("tok"), lax.axis_size("tp")
    line = tok_count // QUAD
    tok_dev, width = query.shape
    kv_here = keys_values.shape[1] // (2 * HEAD)
    columns = column_local.shape[1]
    vmem = pl.BlockSpec(memory_space=pltpu.VMEM)
    dma = pltpu.SemaphoreType.DMA
    f32 = jnp.float32
    return pl.pallas_call(
        functools.partial(back_kernel, line, tp_count, kv_here),
        out_shape=(
            jax.ShapeDtypeStruct((tok_dev, width), jnp.bfloat16),
            jax.ShapeDtypeStruct((1, width), f32),
            jax.ShapeDtypeStruct((1, columns), f32),
        ),
        in_specs=[vmem] * 5,
        out_specs=(vmem,) * 3,
        scratch_shapes=[
            pltpu.VMEM((tok_dev * tok_count, keys_values.shape[1]), jnp.bfloat16),
            pltpu.VMEM((tp_count, 1, columns), f32),
            pltpu.VMEM((1, columns), f32),
            pltpu.VMEM((tok_count, 1, columns), f32),
            pltpu.VMEM((1, width), f32),
            pltpu.VMEM((tok_count, 1, width), f32),
        ]
        + [dma((line,))] * 4
        + [dma((2 * line,))] * 2
        + [dma((tp_count,))] * 2
        + [dma((tok_count,))] * 4,
        compiler_params=pltpu.CompilerParams(
            collective_id=1, has_side_effects=True, vmem_limit_bytes=60 * 1024 * 1024
        ),
    )(query, keys_values, doc_mine, doc_all, column_local)


def on_device(hidden, norm_gain, w_query, w_key, w_value, doc_ids):
    tok_dev = hidden.shape[0]
    row_count = w_query.shape[0]
    tp_count = lax.axis_size("tp")
    tok_index = lax.axis_index("tok")
    tp_index = lax.axis_index("tp")
    matrices = (w_query, w_key, w_value)
    states = hidden.astype(jnp.float32)
    normed = (
        states
        * lax.rsqrt(jnp.mean(states * states, axis=1, keepdims=True) + 1e-05)
        * norm_gain[None, :]
    ).astype(jnp.bfloat16)
    lanes = -tok_dev % 128
    doc_row = jnp.pad(doc_ids, (0, lanes))[None]
    positions = (tok_index * tok_dev + jnp.arange(tok_dev, dtype=jnp.int32)).astype(
        jnp.float32
    )
    query, keys_values, peaks, docs, *relaid = front(
        normed, doc_row, *rotation(positions), matrices
    )
    doc_all = docs[:, 0, :tok_dev].reshape(1, -1)
    sub_rows = row_count // tp_count
    smooth_part = smooth_from(
        lax.dynamic_slice_in_dim(
            peaks[0], (tok_index % QUAD) * row_count + tp_index * sub_rows, sub_rows
        ),
        functools.reduce(
            jnp.maximum, [jnp.max(jnp.abs(block), axis=1) for block in relaid]
        ).astype(jnp.float32),
    )
    column_local = jnp.concatenate(
        [
            jnp.max(jnp.abs(smooth_part[:, None] * block.astype(jnp.float32)), axis=0)
            for block in relaid
        ]
    )
    attended, out_scale, column_scales = back(
        query,
        keys_values,
        doc_ids[:, None],
        doc_all,
        column_local[None],
    )
    out_scale = out_scale[0]
    every = column_scales[0]
    every_scale = jnp.split(
        every, [relaid[0].shape[1], relaid[0].shape[1] + relaid[1].shape[1]]
    )
    scales = tuple(
        lax.dynamic_slice_in_dim(scale, tp_index * matrix.shape[1], matrix.shape[1])
        for scale, matrix in zip(every_scale, matrices)
    )
    gain_part = lax.dynamic_slice_in_dim(
        norm_gain, tok_index * row_count + tp_index * sub_rows, sub_rows
    )
    folded_gain = gain_part / smooth_part
    codes = tuple(
        (
            smooth_part[:, None] * block.astype(jnp.float32) / column_scale[None, :]
            for block, column_scale in zip(relaid, every_scale)
        )
    )
    return (
        attended,
        out_scale,
        folded_gain,
        codes[0],
        codes[1],
        codes[2],
        scales[0],
        scales[1],
        scales[2],
    )


def solution(mesh):
    in_specs = (P("tok", None), P(), P("tok", "tp"), P("tok", "tp"), P("tok", "tp"), P("tok"))
    out_specs = (
        P("tok", "tp"),
        P("tp"),
        P(("tok", "tp")),
        P(("tok", "tp"), None),
        P(("tok", "tp"), None),
        P(("tok", "tp"), None),
        P("tp"),
        P("tp"),
        P("tp"),
    )
    return jax.shard_map(
        on_device, mesh=mesh, in_specs=in_specs, out_specs=out_specs, check_vma=False
    )
```
